256 devices in a mesh: expert: 64 (over x, z, core), dp: 4 (over y).
Axes of the slice: x: 4, y: 4, z: 8, core: 2. Of those that a mesh axis runs over, the one named last changes fastest.
Arguments:
- tokens: bfloat16 [65536, 2048], P(('expert', 'dp')), may hold values from -256 to 256
- routes: int32 [65536, 2], P(('expert', 'dp')), may hold values from 0 to 255, all different within a row
- priority: int32 [256, 256], P(('expert', 'dp')), may hold values from 0 to 255, each once within a row
- router: bfloat16 [2048, 256], replicated, may hold values from -3 to 3
- w_in: bfloat16 [256, 2048, 1024], P(('expert', 'dp')), may hold values from -0.125 to 0.125
- w_out: bfloat16 [256, 2048, 1024], P(('expert', 'dp')), may hold values from -0.1875 to 0.1875
Outputs:
- mixed: bfloat16 [65536, 2048], P(('expert', 'dp'))
- aux_loss: float32 [], replicated
The draws below stay inside these ranges and needn't reach their ends.
Inputs may be any that keep to these rules, and one draw needn't show every extreme that they name: `routes`: a token's two experts differ; every expert is named by some token. `priority`: each group's 256 tokens hold every rank once.
All inputs are finite; a program needn't handle non-finite values.
Results may differ from the reference program's by a relative error of at most 0.0014.
The reference program's roundings to bfloat16 on the way count: a program that leaves them out, or rounds other values in their place, can miss the bound.
Values may be sent and summed in bfloat16 or wider, within the bound.
A program may use at most 64 MiB of HBM per device.

```python
import math
import jax
import jax.numpy as jnp
from jax import lax

D = 2048
FF = 1024
TOK_DEV = 256
EXPERTS = 256
GROUPS = 256
TOKENS = 65536
CAP = 4


def router_values(key):
    sub_key = jax.random.fold_in(key, 71)
    spread = 3.0 / math.sqrt(D)
    values = jnp.clip(jax.random.normal(sub_key, (D, EXPERTS), jnp.float32), -6.0, 6.0) * spread
    return values


def draw_router(key, part):
    return router_values(key).astype(jnp.bfloat16)


def draw_tokens(key, part):
    base = jnp.clip(jax.random.normal(jax.random.fold_in(key, 5), (TOKENS, D), jnp.float32), -6.0, 6.0)
    return base.astype(jnp.bfloat16)


def block_scale(own_key, dims, cuts, low, top_value):
    gain, own = 1.0, jax.random.fold_in(own_key, 6)
    for position, parts in cuts:
        draws = jnp.exp(jax.random.uniform(jax.random.fold_in(own, position), (parts,), jnp.float32, low / len(cuts), top_value / len(cuts)))
        gain = gain * jnp.repeat(draws, dims[position] // parts).reshape([-1 if axis == position else 1 for axis in range(len(dims))])
    return gain


def distinct(rng, rows, count, top, lift):
    sequence = jax.random.permutation(jax.random.fold_in(rng, 1), count)
    favour = sequence
    for power in range(3):
        favour = favour * favour // count
    favour = favour * lift // count
    chance = jax.random.randint(jax.random.fold_in(rng, 2), (rows, count), 0, 4096) + favour
    fixed_rows = jax.random.permutation(jax.random.fold_in(rng, 3), rows)[jnp.arange(count) % rows]
    chance = jnp.where(jnp.arange(rows)[:, None] == fixed_rows[None, :], 1 << 14, chance)
    score = chance * count + jnp.arange(count)
    return lax.top_k(score.astype(jnp.int32), top)[1].astype(jnp.int32)


def noise(key, dims, width, bound, pieces=(), kind=jnp.bfloat16):
    level = block_scale(key, dims, pieces, -0.22, 0.18) if pieces else 1.0
    entries = jax.random.normal(key, dims, jnp.float32) * width * level
    return jnp.minimum(jnp.maximum(entries, -bound), bound).astype(kind)


def setup_inputs(seed: int = 0) -> dict:
    arg_keys = jax.random.split(jax.random.key(seed), 7)
    return {
        "tokens": draw_tokens(jax.random.fold_in(arg_keys[6], 71), 0),
        "routes": distinct(arg_keys[1], TOKENS, EXPERTS, 2, 64),
        "priority": jax.vmap(lambda own: jax.random.permutation(own, TOK_DEV))(jax.random.split(arg_keys[2], GROUPS)).reshape((GROUPS, TOK_DEV)).astype(jnp.int32),
        "router": draw_router(jax.random.fold_in(arg_keys[6], 71), 0),
        "w_in": noise(arg_keys[4], (EXPERTS, D, FF), D ** -0.5, 0.125, ((0, 256),)),
        "w_out": noise(arg_keys[5], (EXPERTS, D, FF), FF ** -0.5, 0.1875, ((0, 256),)),
    }


def reference(tokens, routes, priority, router, w_in, w_out):
    group_count = TOKENS // TOK_DEV
    logits = jnp.dot(tokens, router, preferred_element_type=jnp.float32)
    probs = jax.nn.softmax(logits, axis=-1)
    first = routes[:, 0].astype(jnp.int32)
    second = routes[:, 1].astype(jnp.int32)
    logit_first = jnp.take_along_axis(logits, first[:, None], axis=1)[:, 0]
    logit_second = jnp.take_along_axis(logits, second[:, None], axis=1)[:, 0]
    gate_first = jax.nn.sigmoid(logit_first - logit_second).astype(jnp.bfloat16)
    gate_second = jax.nn.sigmoid(logit_second - logit_first).astype(jnp.bfloat16)
    expert_ids = jnp.arange(EXPERTS, dtype=jnp.int32)
    first_grouped = first.reshape(group_count, TOK_DEV)
    second_grouped = second.reshape(group_count, TOK_DEV)

    def positions(items):
        first_row, second_row, ranks = items
        first_hot = (first_row[:, None] == expert_ids[None, :]).astype(jnp.float32)
        second_hot = (second_row[:, None] == expert_ids[None, :]).astype(jnp.float32)
        earlier = (ranks[None, :] < ranks[:, None]).astype(jnp.float32)
        before_first = jnp.dot(earlier, first_hot, preferred_element_type=jnp.float32)
        before_second = jnp.dot(earlier, second_hot, preferred_element_type=jnp.float32)
        first_load = jnp.sum(first_hot, axis=0)
        pos_first = jnp.sum(before_first * first_hot, axis=1)
        pos_second = jnp.sum((before_second + first_load[None, :]) * second_hot, axis=1)
        return pos_first.astype(jnp.int32), pos_second.astype(jnp.int32)

    pos_first, pos_second = lax.map(positions, (first_grouped, second_grouped, priority))
    dump_slot = CAP * EXPERTS
    slot_first = jnp.where(pos_first < CAP, pos_first * EXPERTS + first_grouped, dump_slot).astype(jnp.int32)
    slot_second = jnp.where(pos_second < CAP, pos_second * EXPERTS + second_grouped, dump_slot).astype(jnp.int32)
    grouped_tokens = tokens.reshape(group_count, TOK_DEV, D)

    def fill(items):
        rows, first_slots, second_slots = items
        buffer = jnp.zeros((dump_slot + 1, D), jnp.bfloat16)
        buffer = buffer.at[first_slots].set(rows).at[second_slots].set(rows)
        return buffer[:dump_slot]

    buffers = lax.map(fill, (grouped_tokens, slot_first, slot_second))
    by_expert = buffers.reshape(group_count, CAP, EXPERTS, D).transpose(2, 0, 1, 3).reshape(EXPERTS, group_count * CAP, D)

    def expert_ffn(items):
        rows, weight_in, weight_out = items
        hidden = jax.nn.relu(jnp.dot(rows, weight_in, preferred_element_type=jnp.float32)).astype(jnp.bfloat16)
        return jnp.dot(hidden, weight_out.T, preferred_element_type=jnp.float32).astype(jnp.bfloat16)

    produced = lax.map(expert_ffn, (by_expert, w_in, w_out))
    returned = produced.reshape(EXPERTS, group_count, CAP, D).transpose(1, 2, 0, 3).reshape(group_count, dump_slot, D)
    returned = jnp.concatenate([returned, jnp.zeros((group_count, 1, D), jnp.bfloat16)], axis=1)

    def combine(items):
        table, first_slots, second_slots, weight_first, weight_second = items
        rows_first = table[first_slots].astype(jnp.float32)
        rows_second = table[second_slots].astype(jnp.float32)
        total = weight_first.astype(jnp.float32)[:, None] * rows_first + weight_second.astype(jnp.float32)[:, None] * rows_second
        return total.astype(jnp.bfloat16)

    mixed = lax.map(combine, (returned, slot_first, slot_second, gate_first.reshape(group_count, TOK_DEV), gate_second.reshape(group_count, TOK_DEV)))
    mixed = mixed.reshape(TOKENS, D)
    mean_prob = jnp.mean(probs, axis=0)
    first_share = jnp.mean((first[:, None] == expert_ids[None, :]).astype(jnp.float32), axis=0)
    aux_loss = EXPERTS * jnp.sum(mean_prob * first_share)
    return mixed, aux_loss
```

```python
import jax
import jax.numpy as jnp
from jax import lax
from jax.experimental import pallas as pl
from jax.experimental.pallas import tpu as pltpu
from jax.sharding import Mesh
from jax.sharding import PartitionSpec as P

MESH = pl.DeviceIdType.MESH
EXPERT_DP = ("expert_0", "expert_1", "expert_2", "dp")
BF = jnp.bfloat16
F32 = jnp.float32
D = 2048
FF = 1024
NC = 4
L = D // NC
NONE = -1.0e6

S0 = 0
S1 = 768
S2 = S1 + 2 * 512
RX = S2 + 2 * 640
RB_ROWS = RX + 3 * 128


def iota(shape, dim):
    return lax.broadcasted_iota(jnp.int32, shape, dim)


def rows(start, count):
    return pl.ds(start if isinstance(start, int) else pl.multiple_of(start, 8), count)


def cols(c, width=L):
    return pl.ds(pl.multiple_of(c * width, width), width)


def to_col(row):
    eye = iota((256, 256), 0) == iota((256, 256), 1)
    return jnp.sum(jnp.where(eye, row, 0.0), axis=1, keepdims=True)


def to_row(col):
    eye = iota((256, 256), 0) == iota((256, 256), 1)
    return jnp.sum(jnp.where(eye, col, 0.0), axis=0, keepdims=True)


def kernel(
    t_hbm, routes, ranks, router_hbm, w1_hbm, w2_hbm, out, aux,
    T2, SRC, PK, X, Y, RB, V2, V1, W1, W2, RT, H, PM, PMK, C2, C1, C0, M, STA, STB, STC,
    ld, zs, zr, tws, twr, pks, pkr, ms, mr, xs, xr, ys, yr, sts, str_,
    gs, gr, es, er, t1s, t1r, v2s, v2r, v1s, v1r,
):
    x = lax.axis_index("expert_0")
    z = lax.axis_index("expert_1")
    k = lax.axis_index("expert_2")
    y = lax.axis_index("dp")
    me = x * 4 + y
    kt = 1 - k
    zn = [lax.rem(z + 1, 8), lax.rem(z + 7, 8)]
    zn2 = [lax.rem(z + 2, 8), lax.rem(z + 6, 8)]

    def remote(src, dst, ss, rs, **where):
        return pltpu.make_async_remote_copy(
            src_ref=src, dst_ref=dst, send_sem=ss, recv_sem=rs, device_id=where, device_id_type=MESH
        )

    def xy(i):
        d = lax.rem(me + i, 16)
        return d, {"expert_0": d // 4, "dp": lax.rem(d, 4)}

    loads = [
        pltpu.make_async_copy(t_hbm, T2.at[rows(k * 256, 256)], ld.at[0]),
        pltpu.make_async_copy(router_hbm, RT, ld.at[1]),
        pltpu.make_async_copy(w1_hbm, W1, ld.at[2]),
        pltpu.make_async_copy(w2_hbm, W2, ld.at[3]),
    ]
    for load in loads:
        load.start()

    barrier = pltpu.get_barrier_semaphore()

    @pl.loop(1, 16)
    def _(i):
        pl.semaphore_signal(barrier, inc=1, device_id=xy(i)[1], device_id_type=MESH)

    @pl.loop(1, 8)
    def _(i):
        pl.semaphore_signal(
            barrier, inc=1, device_id={"expert_1": lax.rem(z + i, 8)}, device_id_type=MESH
        )

    for other in (zn[0], zn[1], zn2[0], zn2[1], z):
        pl.semaphore_signal(
            barrier, inc=1, device_id={"expert_1": other, "expert_2": kt}, device_id_type=MESH
        )
    pl.semaphore_wait(barrier, 27)

    def t2(idx, kk):
        return rows((idx * 2 + kk) * 256, 256)

    def tok_z(u, step, c):
        src = t2(0 if step == 0 else 1 + u, k)
        dst = t2(1 + u + 2 * step, k)
        return remote(
            T2.at[src, cols(c)], T2.at[dst, cols(c)], zs.at[u, step, c], zr.at[u, step, c],
            expert_1=zn[u],
        )

    def tok_twin(idx, c):
        r = t2(idx, k)
        return remote(
            T2.at[r, cols(c)], T2.at[r, cols(c)], tws.at[idx, c], twr.at[idx, c], expert_2=kt
        )

    def slots_z(u, far, c):
        if far:
            return remote(
                PK.at[rows(u * 192 + 128, 64), cols(c)], SRC.at[rows(7 * 128 + u * 64, 64), cols(c)],
                pks.at[u, 1, c], pkr.at[u, 1, c], expert_1=zn2[u],
            )
        return remote(
            PK.at[rows(u * 192, 128), cols(c)], SRC.at[rows((5 + u) * 128, 128), cols(c)],
            pks.at[u, 0, c], pkr.at[u, 0, c], expert_1=zn[u],
        )

    def meta_to(n):
        src = M.at[rows(k * 8, 8)]
        if n == 0:
            idx, where = 0, {"expert_2": kt}
        else:
            idx, other = (n - 1) // 2 + 1, (n - 1) % 2
            target = (zn if idx < 3 else zn2)[(idx - 1) % 2]
            where = {"expert_1": target, "expert_2": kt if other else k}
        return remote(src, M.at[rows((idx * 2 + k) * 8, 8)], ms.at[n], mr.at[idx * 2 + k], **where)

    def meta_wait(idx):
        for kk in ((kt,) if idx == 0 else (0, 1)):
            r = rows((idx * 2 + kk) * 8, 8)
            remote(M.at[r], M.at[r], ms.at[0], mr.at[idx * 2 + kk], expert_2=kt).wait_recv()

    def tile_out(idx, i):
        d, where = xy(i)
        return remote(
            SRC.at[rows(idx * 128 + d * 8, 8)], X.at[rows(idx * 128 + me * 8, 8)],
            xs.at[idx], xr.at[idx], **where,
        )

    def tiles(idx):
        r = rows(idx * 128, 120)
        return remote(SRC.at[r], X.at[r], xs.at[idx], xr.at[idx], expert_2=kt)

    def scatter(idx):
        @pl.loop(1, 16)
        def _(i):
            tile_out(idx, i).start()

        own = rows(idx * 128 + me * 8, 8)
        X[own, :] = SRC[own, :]

    def home_row(idx):
        if idx == 0:
            return S0 + k * 128
        if idx < 3:
            return S1 + (idx - 1) * 512 + k * 128
        if idx < 5:
            return S2 + (idx - 3) * 640 + k * 320
        return RX + (idx - 5) * 128

    def tile_back(idx, i):
        d, where = xy(i)
        return remote(
            Y.at[rows(idx * 128 + d * 8, 8)], RB.at[rows(home_row(idx) + me * 8, 8)],
            ys.at[idx], yr.at[idx], **where,
        )

    def tiles_back(idx):
        return remote(
            Y.at[rows(idx * 128, 120)], RB.at[rows(home_row(idx), 120)], ys.at[idx], yr.at[idx],
            expert_2=kt,
        )

    def scatter_back(idx):
        @pl.loop(1, 16)
        def _(i):
            tile_back(idx, i).start()

        RB[rows(home_row(idx) + me * 8, 8), :] = Y[rows(idx * 128 + me * 8, 8), :]

    def back_z(d, far, c):
        if far:
            return remote(
                RB.at[rows(RX + 256 + d * 64, 64), cols(c)],
                RB.at[rows(S2 + d * 640 + k * 320 + 256, 64), cols(c)],
                gs.at[d, 1, c], gr.at[d, 1, c], expert_1=zn2[1 - d],
            )
        return remote(
            RB.at[rows(RX + d * 128, 128), cols(c)],
            RB.at[rows(S2 + d * 640 + k * 320 + 128, 128), cols(c)],
            gs.at[d, 0, c], gr.at[d, 0, c], expert_1=zn[1 - d],
        )

    def back_twin2(d, c):
        r = rows(S2 + d * 640 + k * 320, 320)
        return remote(RB.at[r, cols(c)], RB.at[r, cols(c)], es.at[d, c], er.at[d, c], expert_2=kt)

    def back_twin1(n):
        r = rows(home_row(n), 128)
        return remote(RB.at[r], RB.at[r], t1s.at[n], t1r.at[n], expert_2=kt)

    def mixed2(d, c):
        return remote(
            V2.at[rows(d * 256, 256), cols(c)], RB.at[rows(S1 + d * 512 + 256, 256), cols(c)],
            v2s.at[d, c], v2r.at[d, c], expert_1=zn[1 - d],
        )

    def mixed1(d, c):
        return remote(
            V1.at[rows(d * 256, 256), cols(c)], RB.at[rows(S0 + 256 + d * 256, 256), cols(c)],
            v1s.at[d, c], v1r.at[d, c], expert_1=zn[1 - d],
        )

    def stat_xy(i):
        _, where = xy(i)
        r = rows(me * 8, 8)
        return remote(STA.at[r], STA.at[r], sts.at[0], str_.at[0], **where)

    def stat_z(i):
        r = rows(z * 8, 8)
        return remote(
            STB.at[r], STB.at[r], sts.at[1], str_.at[1], expert_1=lax.rem(z + i, 8)
        )

    def stat_twin():
        r = rows(k * 8, 8)
        return remote(STC.at[r], STC.at[r], sts.at[2], str_.at[2], expert_2=kt)

    def one_hot(dst, row0, count, idx, base):
        code = (iota((count, 256), 0) + base).astype(F32)
        for g in range(2):
            r = (idx * 2 + g) * 8
            hit = (code == M[r : r + 1, :]) | (code == M[r + 1 : r + 2, :])
            dst[row0 : row0 + count, g * 256 : (g + 1) * 256] = jnp.where(hit, 1.0, 0.0).astype(BF)

    def pack(idx):
        one_hot(PM, 0, 128, idx, (z * 2 + k) * 128)

        @pl.loop(0, NC)
        def _(c):
            SRC[idx * 128 : idx * 128 + 128, cols(c)] = jnp.dot(
                PM[...], T2[idx * 512 : idx * 512 + 512, cols(c)], preferred_element_type=F32
            ).astype(BF)

    def ffn(idx, count):
        r = pl.ds(idx * 128, count * 128)
        h = pl.ds(0, count * 128)

        @pl.loop(0, FF // 256)
        def _(n):
            part = jnp.dot(X[r, :], W1[:, cols(n, 256)], preferred_element_type=F32)
            H[h, cols(n, 256)] = jnp.maximum(part, 0.0).astype(BF)

        @pl.loop(0, D // 256)
        def _(n):
            Y[r, cols(n, 256)] = lax.dot_general(
                H[h, :], W2[pl.ds(pl.multiple_of(n * 256, 256), 256), :],
                (((1,), (1,)), ((), ())), preferred_element_type=F32,
            ).astype(BF)

    def meta_cols(idx):
        block = M[rows((idx * 2 + k) * 8, 8), :]
        return [to_col(block[i : i + 1, :]) for i in range(6)]

    def weights(e1, e2, low, g1, g2):
        in1 = (e1 >= low) & (e1 <= 4.0)
        in2 = (e2 >= low) & (e2 <= 4.0)
        both = in1 & in2
        return jnp.where(both, g1, 1.0), jnp.where(both, g2, 1.0)

    def passed(e1, e2, low, w1, w2):
        in1 = (e1 >= low) & (e1 <= 4.0)
        in2 = (e2 >= low) & (e2 <= 4.0)
        return jnp.where(
            in1 & in2, 1.0, jnp.where(in1, w1, 0.0) + jnp.where(in2, w2, 0.0)
        )

    def placed(code, s1, s2, w1, w2):
        return (jnp.where(code == s1, w1, 0.0) + jnp.where(code == s2, w2, 0.0)).astype(BF)

    def diagonal(col):
        eye = iota((256, 256), 0) == iota((256, 256), 1)
        return jnp.where(eye, col, 0.0).astype(BF)

    loads[0].wait()

    @pl.loop(0, NC)
    def _(c):
        tok_z(0, 0, c).start()
        tok_z(1, 0, c).start()
        tok_twin(0, c).start()

    loads[1].wait()
    logits = jnp.dot(T2[t2(0, k), :], RT[...], preferred_element_type=F32)
    lane = iota((256, 256), 1).astype(F32)
    first_row, second_row = routes[0:1, :], routes[1:2, :]
    first_hot = jnp.where(lane == to_col(first_row.astype(F32)), 1.0, 0.0)
    second_hot = jnp.where(lane == to_col(second_row.astype(F32)), 1.0, 0.0)
    logit_first = jnp.sum(logits * first_hot, axis=1, keepdims=True)
    logit_second = jnp.sum(logits * second_hot, axis=1, keepdims=True)
    gate_first = 1.0 / (1.0 + jnp.exp(logit_second - logit_first))
    gate_second = 1.0 / (1.0 + jnp.exp(logit_first - logit_second))
    rank_row = ranks[...].astype(F32)
    earlier = jnp.where(rank_row < to_col(rank_row), 1.0, 0.0).astype(BF)
    before_first = jnp.dot(earlier, first_hot.astype(BF), preferred_element_type=F32)
    before_second = jnp.dot(earlier, second_hot.astype(BF), preferred_element_type=F32)
    first_load = jnp.sum(first_hot, axis=0, keepdims=True)
    pos_first = to_row(jnp.sum(before_first * first_hot, axis=1, keepdims=True))
    pos_second = to_row(
        jnp.sum((before_second + first_load) * second_hot, axis=1, keepdims=True)
    )

    def slot_and_side(expert, pos):
        ex, ez, ek, ey = expert >> 6, (expert >> 3) & 7, (expert >> 2) & 1, expert & 3
        base = (ez * 2 + ek) * 128 + (ex * 4 + ey) * 8 + k * 4
        away = (ez - z) & 7
        side = jnp.where(
            away < 4, away, jnp.where((away == 4) & (ex < 2), 4, away - 8)
        )
        kept = pos < 4.0
        return (
            jnp.where(kept, base.astype(F32) + pos, NONE),
            jnp.where(kept, side.astype(F32), 99.0),
        )

    slot1, side1 = slot_and_side(first_row, pos_first)
    slot2, side2 = slot_and_side(second_row, pos_second)
    zero = jnp.zeros((1, 256), F32)
    own_meta = rows(k * 8, 8)
    M[own_meta, :] = jnp.concatenate(
        [
            slot1, slot2, to_row(gate_first).astype(BF).astype(F32),
            to_row(gate_second).astype(BF).astype(F32), side1, side2, zero, zero,
        ],
        axis=0,
    )
    for n in range(9):
        meta_to(n).start()
    top = jnp.max(logits, axis=1, keepdims=True)
    raised = jnp.exp(logits - top)
    probs = raised / jnp.sum(raised, axis=1, keepdims=True)
    prob_sum = jnp.sum(probs, axis=0, keepdims=True)
    STA[rows(me * 8, 8), :] = jnp.concatenate([prob_sum, first_load] + [zero] * 6, axis=0)

    @pl.loop(1, 16)
    def _(i):
        stat_xy(i).start()

    @pl.loop(0, NC)
    def _(c):
        tok_twin(0, c).wait_recv()

    meta_wait(0)
    pack(0)
    scatter(0)

    @pl.loop(0, NC)
    def _(c):
        for u in range(2):
            tok_z(u, 0, c).wait_recv()
            tok_z(u, 1, c).start()
            tok_twin(1 + u, c).start()

    for idx in (1, 2):
        @pl.loop(0, NC)
        def _(c):
            tok_twin(idx, c).wait_recv()

        meta_wait(idx)
        pack(idx)
        scatter(idx)

    remote(STA.at[0:120], STA.at[0:120], sts.at[0], str_.at[0], expert_2=kt).wait_recv()
    STB[rows(z * 8, 8), :] = sum(STA[8 * i : 8 * i + 8, :] for i in range(16))

    @pl.loop(1, 8)
    def _(i):
        stat_z(i).start()

    loads[2].wait()
    loads[3].wait()
    tiles(0).wait_recv()
    ffn(0, 1)
    scatter_back(0)
    for idx in (3, 4):
        meta_wait(idx)
    for u in range(2):
        one_hot(PMK, u * 192, 128, 3 + u, (zn[u] * 2 + k) * 128)
        one_hot(PMK, u * 192 + 128, 64, 3 + u, (zn2[u] * 2 + k) * 128 + u * 64)

    @pl.loop(0, NC)
    def _(c):
        for u in range(2):
            tok_z(u, 1, c).wait_recv()
            tok_twin(3 + u, c).start()
        for u in range(2):
            tok_twin(3 + u, c).wait_recv()
            PK[u * 192 : u * 192 + 192, cols(c)] = jnp.dot(
                PMK[u * 192 : u * 192 + 192, :], T2[(3 + u) * 512 : (4 + u) * 512, cols(c)],
                preferred_element_type=F32,
            ).astype(BF)
            slots_z(u, True, c).start()
            slots_z(u, False, c).start()

    for idx in (3, 4):
        pack(idx)
        scatter(idx)
    for idx in (1, 2):
        tiles(idx).wait_recv()
    ffn(1, 2)
    for idx in (1, 2):
        scatter_back(idx)
    for idx in (3, 4):
        tiles(idx).wait_recv()
    ffn(3, 2)
    for idx in (3, 4):
        scatter_back(idx)

    remote(STB.at[0:56], STB.at[0:56], sts.at[1], str_.at[1], expert_2=kt).wait_recv()
    STC[rows(k * 8, 8), :] = sum(STB[8 * i : 8 * i + 8, :] for i in range(8))
    stat_twin().start()

    for n in range(3):
        tiles_back(n).wait_recv()
        back_twin1(n).start()

    for d in range(2):
        sign = 1.0 if d == 0 else -1.0
        s1, s2, g1, g2, e1, e2 = meta_cols(3 + d)
        e1, e2 = sign * e1, sign * e2
        w1, w2 = weights(e1, e2, 2.0, g1, g2)
        j = iota((1, 640), 1)
        p = jnp.where(j >= 320, 1, 0)
        r = j - 320 * p
        code = p * 128 + jnp.where(
            r < 128, z * 256 + r,
            jnp.where(r < 256, zn[d] * 256 + r - 128, zn2[d] * 256 + d * 64 + r - 256),
        )
        C2[d * 256 : d * 256 + 256, :] = placed(code.astype(F32), s1, s2, w1, w2)
        s1, s2, g1, g2, e1, e2 = meta_cols(1 + d)
        e1, e2 = sign * e1, sign * e2
        w1, w2 = weights(e1, e2, 1.0, g1, g2)
        near = (iota((1, 256), 1) + z * 256).astype(F32)
        C1[d * 256 : d * 256 + 256, 0:256] = placed(near, s1, s2, w1, w2)
        C1[d * 256 : d * 256 + 256, 256:512] = diagonal(passed(e1, e2, 2.0, w1, w2))
    s1, s2, g1, g2, e1, e2 = meta_cols(0)
    near = (iota((1, 256), 1) + z * 256).astype(F32)
    C0[:, 0:256] = placed(near, s1, s2, g1, g2)
    C0[:, 256:512] = diagonal(passed(e1, e2, 1.0, g1, g2))
    C0[:, 512:768] = diagonal(passed(-e1, -e2, 1.0, g1, g2))

    for u in range(2):
        @pl.loop(0, NC)
        def _(c):
            slots_z(u, True, c).wait_recv()

    scatter(7)
    for u in range(2):
        @pl.loop(0, NC)
        def _(c):
            slots_z(u, False, c).wait_recv()

        scatter(5 + u)
    for idx in (5, 6):
        tiles(idx).wait_recv()
    ffn(5, 2)
    for idx in (5, 6):
        scatter_back(idx)
    tiles(7).wait_recv()
    ffn(7, 1)
    scatter_back(7)

    for d in range(2):
        tiles_back(5 + d).wait_recv()

        @pl.loop(0, NC)
        def _(c):
            back_z(d, False, c).start()

    tiles_back(7).wait_recv()

    @pl.loop(0, NC)
    def _(c):
        back_z(0, True, c).start()
        back_z(1, True, c).start()

    for d in range(2):
        tiles_back(3 + d).wait_recv()

    @pl.loop(0, NC)
    def _(c):
        for d in range(2):
            back_z(d, False, c).wait_recv()
            back_z(d, True, c).wait_recv()
            back_twin2(d, c).start()
        for d in range(2):
            back_twin2(d, c).wait_recv()
            V2[d * 256 : d * 256 + 256, cols(c)] = jnp.dot(
                C2[d * 256 : d * 256 + 256, :], RB[S2 + d * 640 : S2 + d * 640 + 640, cols(c)],
                preferred_element_type=F32,
            ).astype(BF)
            mixed2(d, c).start()

    for n in range(3):
        back_twin1(n).wait_recv()

    @pl.loop(0, NC)
    def _(c):
        for d in range(2):
            mixed2(d, c).wait_recv()
            V1[d * 256 : d * 256 + 256, cols(c)] = jnp.dot(
                C1[d * 256 : d * 256 + 256, :], RB[S1 + d * 512 : S1 + d * 512 + 512, cols(c)],
                preferred_element_type=F32,
            ).astype(BF)
            mixed1(d, c).start()

    stat_twin().wait_recv()
    total = STC[0:8, :] + STC[8:16, :]
    count = 65536.0
    share = (total[0:1, :] / count) * (total[1:2, :] / count)
    aux[...] = jnp.broadcast_to(256.0 * jnp.sum(share, axis=1, keepdims=True), (8, 128))

    @pl.loop(0, NC)
    def _(c):
        for d in range(2):
            mixed1(d, c).wait_recv()
        out[:, cols(c)] = jnp.dot(
            C0[...], RB[S0 : S0 + 768, cols(c)], preferred_element_type=F32
        ).astype(BF)

    @pl.loop(0, NC)
    def _(c):
        for u in range(2):
            tok_z(u, 0, c).wait_send()
            tok_z(u, 1, c).wait_send()
            slots_z(u, False, c).wait_send()
            slots_z(u, True, c).wait_send()
            back_z(u, False, c).wait_send()
            back_z(u, True, c).wait_send()
            back_twin2(u, c).wait_send()
            mixed2(u, c).wait_send()
            mixed1(u, c).wait_send()
        for idx in range(5):
            tok_twin(idx, c).wait_send()

    for n in range(9):
        meta_to(n).wait_send()
    for n in range(3):
        back_twin1(n).wait_send()
    for idx in range(8):
        tiles(idx).wait_send()
        tiles_back(idx).wait_send()
    remote(STA.at[0:120], STA.at[0:120], sts.at[0], str_.at[0], expert_2=kt).wait_send()
    remote(STB.at[0:56], STB.at[0:56], sts.at[1], str_.at[1], expert_2=kt).wait_send()
    stat_twin().wait_send()


def shards(tokens, routes, priority, router, w_in, w_out):
    anywhere = pl.BlockSpec(memory_space=pl.ANY)
    vmem = pl.BlockSpec(memory_space=pltpu.VMEM)
    dma = pltpu.SemaphoreType.DMA
    mixed, aux = pl.pallas_call(
        kernel,
        out_shape=(
            jax.ShapeDtypeStruct((256, D), BF),
            jax.ShapeDtypeStruct((8, 128), F32),
        ),
        in_specs=[anywhere, vmem, vmem, anywhere, anywhere, anywhere],
        out_specs=(vmem, vmem),
        scratch_shapes=[
            pltpu.VMEM((10 * 256, D), BF),
            pltpu.VMEM((8 * 128, D), BF),
            pltpu.VMEM((2 * 192, D), BF),
            pltpu.VMEM((8 * 128, D), BF),
            pltpu.VMEM((8 * 128, D), BF),
            pltpu.VMEM((RB_ROWS, D), BF),
            pltpu.VMEM((2 * 256, D), BF),
            pltpu.VMEM((2 * 256, D), BF),
            pltpu.VMEM((D, FF), BF),
            pltpu.VMEM((D, FF), BF),
            pltpu.VMEM((D, 256), BF),
            pltpu.VMEM((256, FF), BF),
            pltpu.VMEM((128, 512), BF),
            pltpu.VMEM((2 * 192, 512), BF),
            pltpu.VMEM((2 * 256, 640), BF),
            pltpu.VMEM((2 * 256, 512), BF),
            pltpu.VMEM((256, 768), BF),
            pltpu.VMEM((10 * 8, 256), F32),
            pltpu.VMEM((16 * 8, 256), F32),
            pltpu.VMEM((8 * 8, 256), F32),
            pltpu.VMEM((2 * 8, 256), F32),
            dma((4,)),
            dma((2, 2, NC)), dma((2, 2, NC)),
            dma((5, NC)), dma((5, NC)),
            dma((2, 2, NC)), dma((2, 2, NC)),
            dma((9,)), dma((10,)),
            dma((8,)), dma((8,)),
            dma((8,)), dma((8,)),
            dma((3,)), dma((3,)),
            dma((2, 2, NC)), dma((2, 2, NC)),
            dma((2, NC)), dma((2, NC)),
            dma((3,)), dma((3,)),
            dma((2, NC)), dma((2, NC)),
            dma((2, NC)), dma((2, NC)),
        ],
        compiler_params=pltpu.CompilerParams(
            collective_id=0, has_side_effects=True, vmem_limit_bytes=64_000_000
        ),
    )(tokens, routes.T, priority, router, w_in[0], w_out[0])
    return mixed, aux[0, 0]


def solution(mesh):
    torus = Mesh(mesh.devices.reshape(4, 8, 2, mesh.shape["dp"]), EXPERT_DP)
    in_specs = (
        P(EXPERT_DP, None),
        P(EXPERT_DP, None),
        P(EXPERT_DP, None),
        P(),
        P(EXPERT_DP, None, None),
        P(EXPERT_DP, None, None),
    )
    return jax.shard_map(
        shards, mesh=torus, in_specs=in_specs, out_specs=(P(EXPERT_DP, None), P()), check_vma=False
    )
```

```python
import jax
import jax.numpy as jnp
from jax import lax
from jax.experimental import pallas as pl
from jax.experimental.pallas import tpu as pltpu
from jax.sharding import Mesh
from jax.sharding import PartitionSpec as P

MESH = pl.DeviceIdType.MESH
EXPERT_DP = ("expert_0", "expert_1", "expert_2", "dp")
BF = jnp.bfloat16
F32 = jnp.float32
D = 2048
FF = 1024
NC = 4
L = D // NC
NONE = -1.0e6

S0 = 0
S1 = 768
S2 = S1 + 2 * 512
RX = S2 + 2 * 640
RB_ROWS = RX + 3 * 128


def iota(shape, dim):
    return lax.broadcasted_iota(jnp.int32, shape, dim)


def rows(start, count):
    return pl.ds(start if isinstance(start, int) else pl.multiple_of(start, 8), count)


def cols(c, width=L):
    return pl.ds(pl.multiple_of(c * width, width), width)


def to_col(row):
    eye = iota((256, 256), 0) == iota((256, 256), 1)
    return jnp.sum(jnp.where(eye, row, 0.0), axis=1, keepdims=True)


def to_row(col):
    eye = iota((256, 256), 0) == iota((256, 256), 1)
    return jnp.sum(jnp.where(eye, col, 0.0), axis=0, keepdims=True)


def kernel(
    t_hbm, routes, ranks, router_hbm, w1_hbm, w2_hbm, out, aux,
    T2, SRC, PK, X, Y, RB, V2, V1, W1, W2, RT, H, PM, PMK, C2, C1, C0, M, STA, STB, STC,
    ld, zs, zr, tws, twr, pks, pkr, ms, mr, xs, xr, ys, yr, sts, str_,
    gs, gr, es, er, t1s, t1r, v2s, v2r, v1s, v1r,
):
    x = lax.axis_index("expert_0")
    z = lax.axis_index("expert_1")
    k = lax.axis_index("expert_2")
    y = lax.axis_index("dp")
    me = x * 4 + y
    kt = 1 - k
    zn = [lax.rem(z + 1, 8), lax.rem(z + 7, 8)]
    zn2 = [lax.rem(z + 2, 8), lax.rem(z + 6, 8)]

    def remote(src, dst, ss, rs, **where):
        return pltpu.make_async_remote_copy(
            src_ref=src, dst_ref=dst, send_sem=ss, recv_sem=rs, device_id=where, device_id_type=MESH
        )

    def xy(i):
        d = lax.rem(me + i, 16)
        dx = lax.div(d, 4)
        return d, {"expert_0": dx, "dp": d - 4 * dx}

    loads = [
        pltpu.make_async_copy(t_hbm, T2.at[rows(k * 256, 256)], ld.at[0]),
        pltpu.make_async_copy(router_hbm, RT, ld.at[1]),
        pltpu.make_async_copy(w1_hbm, W1, ld.at[2]),
        pltpu.make_async_copy(w2_hbm, W2, ld.at[3]),
    ]
    for load in loads:
        load.start()

    barrier = pltpu.get_barrier_semaphore()

    @pl.loop(1, 16)
    def _(i):
        pl.semaphore_signal(barrier, inc=1, device_id=xy(i)[1], device_id_type=MESH)

    @pl.loop(1, 8)
    def _(i):
        pl.semaphore_signal(
            barrier, inc=1, device_id={"expert_1": lax.rem(z + i, 8)}, device_id_type=MESH
        )

    for other in (zn[0], zn[1], zn2[0], zn2[1], z):
        pl.semaphore_signal(
            barrier, inc=1, device_id={"expert_1": other, "expert_2": kt}, device_id_type=MESH
        )
    pl.semaphore_wait(barrier, 27)

    def t2(idx, kk):
        return rows((idx * 2 + kk) * 256, 256)

    def tok_z(u, step, c):
        src = t2(0 if step == 0 else 1 + u, k)
        dst = t2(1 + u + 2 * step, k)
        return remote(
            T2.at[src, cols(c)], T2.at[dst, cols(c)], zs.at[u, step, c], zr.at[u, step, c],
            expert_1=zn[u],
        )

    def tok_twin(idx, c):
        r = t2(idx, k)
        return remote(
            T2.at[r, cols(c)], T2.at[r, cols(c)], tws.at[idx, c], twr.at[idx, c], expert_2=kt
        )

    def slots_z(u, far, c):
        if far:
            return remote(
                PK.at[rows(u * 192 + 128, 64), cols(c)], SRC.at[rows(7 * 128 + u * 64, 64), cols(c)],
                pks.at[u, 1, c], pkr.at[u, 1, c], expert_1=zn2[u],
            )
        return remote(
            PK.at[rows(u * 192, 128), cols(c)], SRC.at[rows((5 + u) * 128, 128), cols(c)],
            pks.at[u, 0, c], pkr.at[u, 0, c], expert_1=zn[u],
        )

    def meta_to(n):
        src = M.at[rows(k * 8, 8)]
        if n == 0:
            idx, where = 0, {"expert_2": kt}
        else:
            idx, other = (n - 1) // 2 + 1, (n - 1) % 2
            target = (zn if idx < 3 else zn2)[(idx - 1) % 2]
            where = {"expert_1": target, "expert_2": kt if other else k}
        return remote(src, M.at[rows((idx * 2 + k) * 8, 8)], ms.at[n], mr.at[idx * 2 + k], **where)

    def meta_wait(idx):
        for kk in ((kt,) if idx == 0 else (0, 1)):
            r = rows((idx * 2 + kk) * 8, 8)
            remote(M.at[r], M.at[r], ms.at[0], mr.at[idx * 2 + kk], expert_2=kt).wait_recv()

    def tile_out(idx, i, c):
        d, where = xy(i)
        return remote(
            SRC.at[rows(idx * 128 + d * 8, 8), cols(c)],
            X.at[rows(idx * 128 + me * 8, 8), cols(c)],
            xs.at[idx], xr.at[idx], **where,
        )

    def tiles(idx):
        r = rows(idx * 128, 120)
        return remote(SRC.at[r], X.at[r], xs.at[idx], xr.at[idx], expert_2=kt)

    def scatter(idxs, c):
        @pl.loop(1, 16)
        def _(i):
            for idx in idxs:
                tile_out(idx, i, c).start()

        for idx in idxs:
            own = rows(idx * 128 + me * 8, 8)
            X[own, cols(c)] = SRC[own, cols(c)]

    def home_row(idx):
        if idx == 0:
            return S0 + k * 128
        if idx < 3:
            return S1 + (idx - 1) * 512 + k * 128
        if idx < 5:
            return S2 + (idx - 3) * 640 + k * 320
        return RX + (idx - 5) * 128

    def tile_back(idx, i, c):
        d, where = xy(i)
        return remote(
            Y.at[rows(idx * 128 + d * 8, 8), cols(c)],
            RB.at[rows(home_row(idx) + me * 8, 8), cols(c)],
            ys.at[idx, c], yr.at[idx, c], **where,
        )

    def tiles_back(idx, c):
        return remote(
            Y.at[rows(idx * 128, 120), cols(c)], RB.at[rows(home_row(idx), 120), cols(c)],
            ys.at[idx, c], yr.at[idx, c], expert_2=kt,
        )

    def scatter_back(idxs, c):
        @pl.loop(1, 16)
        def _(i):
            for idx in idxs:
                tile_back(idx, i, c).start()

        for idx in idxs:
            RB[rows(home_row(idx) + me * 8, 8), cols(c)] = Y[
                rows(idx * 128 + me * 8, 8), cols(c)
            ]

    def back_z(d, far, c):
        if far:
            return remote(
                RB.at[rows(RX + 256 + d * 64, 64), cols(c)],
                RB.at[rows(S2 + d * 640 + k * 320 + 256, 64), cols(c)],
                gs.at[d, 1, c], gr.at[d, 1, c], expert_1=zn2[1 - d],
            )
        return remote(
            RB.at[rows(RX + d * 128, 128), cols(c)],
            RB.at[rows(S2 + d * 640 + k * 320 + 128, 128), cols(c)],
            gs.at[d, 0, c], gr.at[d, 0, c], expert_1=zn[1 - d],
        )

    def back_twin2(d, c):
        r = rows(S2 + d * 640 + k * 320, 320)
        return remote(RB.at[r, cols(c)], RB.at[r, cols(c)], es.at[d, c], er.at[d, c], expert_2=kt)

    def back_twin1(n, c):
        r = rows(home_row(n), 128)
        return remote(
            RB.at[r, cols(c)], RB.at[r, cols(c)], t1s.at[n, c], t1r.at[n, c], expert_2=kt
        )

    def mixed2(d, c):
        return remote(
            V2.at[rows(d * 256, 256), cols(c)], RB.at[rows(S1 + d * 512 + 256, 256), cols(c)],
            v2s.at[d, c], v2r.at[d, c], expert_1=zn[1 - d],
        )

    def mixed1(d, c):
        return remote(
            V1.at[rows(d * 256, 256), cols(c)], RB.at[rows(S0 + 256 + d * 256, 256), cols(c)],
            v1s.at[d, c], v1r.at[d, c], expert_1=zn[1 - d],
        )

    def stat_xy(i):
        _, where = xy(i)
        r = rows(me * 8, 8)
        return remote(STA.at[r], STA.at[r], sts.at[0], str_.at[0], **where)

    def stat_z(i):
        r = rows(z * 8, 8)
        return remote(
            STB.at[r], STB.at[r], sts.at[1], str_.at[1], expert_1=lax.rem(z + i, 8)
        )

    def stat_twin():
        r = rows(k * 8, 8)
        return remote(STC.at[r], STC.at[r], sts.at[2], str_.at[2], expert_2=kt)

    def one_hot(dst, row0, count, idx, base):
        code = (iota((count, 256), 0) + base).astype(F32)
        for g in range(2):
            r = (idx * 2 + g) * 8
            hit = (code == M[r : r + 1, :]) | (code == M[r + 1 : r + 2, :])
            dst[row0 : row0 + count, g * 256 : (g + 1) * 256] = jnp.where(hit, 1.0, 0.0).astype(BF)

    def pack(idx, slot, c):
        SRC[idx * 128 : idx * 128 + 128, cols(c)] = jnp.dot(
            PM[slot * 128 : slot * 128 + 128, :], T2[idx * 512 : idx * 512 + 512, cols(c)],
            preferred_element_type=F32,
        ).astype(BF)

    def ffn_in(idx, count):
        r = pl.ds(idx * 128, count * 128)

        @pl.loop(0, FF // 512)
        def _(n):
            part = jnp.dot(X[r, :], W1[:, cols(n, 512)], preferred_element_type=F32)
            H[0 : count * 128, cols(n, 512)] = jnp.maximum(part, 0.0).astype(BF)

    def ffn_out(idx, count, c):
        Y[idx * 128 : (idx + count) * 128, cols(c)] = lax.dot_general(
            H[0 : count * 128, :], W2[cols(c), :],
            (((1,), (1,)), ((), ())), preferred_element_type=F32,
        ).astype(BF)

    def ffn(idx, count):
        ffn_in(idx, count)

        @pl.loop(0, NC)
        def _(c):
            ffn_out(idx, count, c)

    def meta_cols(idx):
        block = M[rows((idx * 2 + k) * 8, 8), :]
        return [to_col(block[i : i + 1, :]) for i in range(6)]

    def weights(e1, e2, low, g1, g2):
        in1 = (e1 >= low) & (e1 <= 4.0)
        in2 = (e2 >= low) & (e2 <= 4.0)
        both = in1 & in2
        return jnp.where(both, g1, 1.0), jnp.where(both, g2, 1.0)

    def passed(e1, e2, low, w1, w2):
        in1 = (e1 >= low) & (e1 <= 4.0)
        in2 = (e2 >= low) & (e2 <= 4.0)
        return jnp.where(
            in1 & in2, 1.0, jnp.where(in1, w1, 0.0) + jnp.where(in2, w2, 0.0)
        )

    def placed(code, s1, s2, w1, w2):
        return (jnp.where(code == s1, w1, 0.0) + jnp.where(code == s2, w2, 0.0)).astype(BF)

    def diagonal(col):
        eye = iota((256, 256), 0) == iota((256, 256), 1)
        return jnp.where(eye, col, 0.0).astype(BF)

    loads[0].wait()

    @pl.loop(0, NC)
    def _(c):
        tok_z(0, 0, c).start()
        tok_z(1, 0, c).start()
        tok_twin(0, c).start()

    loads[1].wait()
    logits = jnp.dot(T2[t2(0, k), :], RT[...], preferred_element_type=F32)
    lane = iota((256, 256), 1).astype(F32)
    first_row, second_row = routes[0:1, :], routes[1:2, :]
    first_hot = jnp.where(lane == to_col(first_row.astype(F32)), 1.0, 0.0)
    second_hot = jnp.where(lane == to_col(second_row.astype(F32)), 1.0, 0.0)
    logit_first = jnp.sum(logits * first_hot, axis=1, keepdims=True)
    logit_second = jnp.sum(logits * second_hot, axis=1, keepdims=True)
    gate_first = 1.0 / (1.0 + jnp.exp(logit_second - logit_first))
    gate_second = 1.0 / (1.0 + jnp.exp(logit_first - logit_second))
    rank_row = ranks[...].astype(F32)
    earlier = jnp.where(rank_row < to_col(rank_row), 1.0, 0.0).astype(BF)
    before_first = jnp.dot(earlier, first_hot.astype(BF), preferred_element_type=F32)
    before_second = jnp.dot(earlier, second_hot.astype(BF), preferred_element_type=F32)
    first_load = jnp.sum(first_hot, axis=0, keepdims=True)
    pos_first = to_row(jnp.sum(before_first * first_hot, axis=1, keepdims=True))
    pos_second = to_row(
        jnp.sum((before_second + first_load) * second_hot, axis=1, keepdims=True)
    )

    def slot_and_side(expert, pos):
        ex, ez, ek, ey = expert >> 6, (expert >> 3) & 7, (expert >> 2) & 1, expert & 3
        base = (ez * 2 + ek) * 128 + (ex * 4 + ey) * 8 + k * 4
        away = (ez - z) & 7
        side = jnp.where(
            away < 4, away, jnp.where((away == 4) & (ex < 2), 4, away - 8)
        )
        kept = pos < 4.0
        return (
            jnp.where(kept, base.astype(F32) + pos, NONE),
            jnp.where(kept, side.astype(F32), 99.0),
        )

    slot1, side1 = slot_and_side(first_row, pos_first)
    slot2, side2 = slot_and_side(second_row, pos_second)
    zero = jnp.zeros((1, 256), F32)
    own_meta = rows(k * 8, 8)
    M[own_meta, :] = jnp.concatenate(
        [
            slot1, slot2, to_row(gate_first).astype(BF).astype(F32),
            to_row(gate_second).astype(BF).astype(F32), side1, side2, zero, zero,
        ],
        axis=0,
    )
    for n in range(9):
        meta_to(n).start()
    top = jnp.max(logits, axis=1, keepdims=True)
    raised = jnp.exp(logits - top)
    probs = raised / jnp.sum(raised, axis=1, keepdims=True)
    prob_sum = jnp.sum(probs, axis=0, keepdims=True)
    STA[rows(me * 8, 8), :] = jnp.concatenate([prob_sum, first_load] + [zero] * 6, axis=0)

    @pl.loop(1, 16)
    def _(i):
        stat_xy(i).start()

    plane = (z * 2 + k) * 128
    meta_wait(0)
    one_hot(PM, 0, 128, 0, plane)

    @pl.loop(0, NC)
    def _(c):
        tok_twin(0, c).wait_recv()
        pack(0, 0, c)
        scatter((0,), c)

    for idx in (1, 2):
        meta_wait(idx)
        one_hot(PM, (idx - 1) * 128, 128, idx, plane)

    @pl.loop(0, NC)
    def _(c):
        for u in range(2):
            tok_z(u, 0, c).wait_recv()
            tok_z(u, 1, c).start()
            tok_twin(1 + u, c).start()
        for u in range(2):
            tok_twin(1 + u, c).wait_recv()
            pack(1 + u, u, c)
        scatter((1, 2), c)

    remote(STA.at[0:120], STA.at[0:120], sts.at[0], str_.at[0], expert_2=kt).wait_recv()
    STB[rows(z * 8, 8), :] = sum(STA[8 * i : 8 * i + 8, :] for i in range(16))

    @pl.loop(1, 8)
    def _(i):
        stat_z(i).start()

    loads[2].wait()
    loads[3].wait()
    for idx in (3, 4):
        meta_wait(idx)
        one_hot(PM, (idx - 3) * 128, 128, idx, plane)
    for u in range(2):
        one_hot(PMK, u * 192, 128, 3 + u, (zn[u] * 2 + k) * 128)
        one_hot(PMK, u * 192 + 128, 64, 3 + u, (zn2[u] * 2 + k) * 128 + u * 64)
    tiles(0).wait_recv()
    ffn_in(0, 1)

    @pl.loop(0, NC)
    def _(c):
        ffn_out(0, 1, c)
        scatter_back((0,), c)

    @pl.loop(0, NC)
    def _(c):
        for u in range(2):
            tok_z(u, 1, c).wait_recv()
            tok_twin(3 + u, c).start()
        for u in range(2):
            tok_twin(3 + u, c).wait_recv()
            PK[u * 192 : u * 192 + 192, cols(c)] = jnp.dot(
                PMK[u * 192 : u * 192 + 192, :], T2[(3 + u) * 512 : (4 + u) * 512, cols(c)],
                preferred_element_type=F32,
            ).astype(BF)
            slots_z(u, True, c).start()
            slots_z(u, False, c).start()
        for u in range(2):
            pack(3 + u, u, c)
        scatter((3, 4), c)

    for idx in (1, 2):
        tiles(idx).wait_recv()
    ffn(1, 2)

    def far_slots(c):
        for u in range(2):
            slots_z(u, True, c).wait_recv()
            slots_z(u, False, c).wait_recv()
        scatter((5, 6, 7), c)

    @pl.loop(0, NC - 1)
    def _(c):
        far_slots(c)

    for idx in (3, 4):
        tiles(idx).wait_recv()
    ffn(3, 2)
    far_slots(NC - 1)

    remote(STB.at[0:56], STB.at[0:56], sts.at[1], str_.at[1], expert_2=kt).wait_recv()
    STC[rows(k * 8, 8), :] = sum(STB[8 * i : 8 * i + 8, :] for i in range(8))
    stat_twin().start()

    @pl.loop(0, NC)
    def _(c):
        tiles_back(0, c).wait_recv()
        back_twin1(0, c).start()

    for d in range(2):
        sign = 1.0 if d == 0 else -1.0
        s1, s2, g1, g2, e1, e2 = meta_cols(3 + d)
        e1, e2 = sign * e1, sign * e2
        w1, w2 = weights(e1, e2, 2.0, g1, g2)
        j = iota((1, 640), 1)
        p = jnp.where(j >= 320, 1, 0)
        r = j - 320 * p
        code = p * 128 + jnp.where(
            r < 128, z * 256 + r,
            jnp.where(r < 256, zn[d] * 256 + r - 128, zn2[d] * 256 + d * 64 + r - 256),
        )
        C2[d * 256 : d * 256 + 256, :] = placed(code.astype(F32), s1, s2, w1, w2)
        s1, s2, g1, g2, e1, e2 = meta_cols(1 + d)
        e1, e2 = sign * e1, sign * e2
        w1, w2 = weights(e1, e2, 1.0, g1, g2)
        near = (iota((1, 256), 1) + z * 256).astype(F32)
        C1[d * 256 : d * 256 + 256, 0:256] = placed(near, s1, s2, w1, w2)
        C1[d * 256 : d * 256 + 256, 256:512] = diagonal(passed(e1, e2, 2.0, w1, w2))
    s1, s2, g1, g2, e1, e2 = meta_cols(0)
    near = (iota((1, 256), 1) + z * 256).astype(F32)
    C0[:, 0:256] = placed(near, s1, s2, g1, g2)
    C0[:, 256:512] = diagonal(passed(e1, e2, 1.0, g1, g2))
    C0[:, 512:768] = diagonal(passed(-e1, -e2, 1.0, g1, g2))

    for idx in (5, 6, 7):
        tiles(idx).wait_recv()
    ffn_in(5, 3)

    @pl.loop(0, NC)
    def _(c):
        ffn_out(5, 3, c)
        scatter_back((5, 6, 7), c)

    @pl.loop(0, NC)
    def _(c):
        for idx in (5, 6, 7):
            tiles_back(idx, c).wait_recv()
        for d in range(2):
            back_z(d, True, c).start()
            back_z(d, False, c).start()
        scatter_back((3, 4), c)

    @pl.loop(0, NC)
    def _(c):
        scatter_back((1, 2), c)

    @pl.loop(0, NC)
    def _(c):
        for d in range(2):
            tiles_back(3 + d, c).wait_recv()
            back_z(d, False, c).wait_recv()
            back_z(d, True, c).wait_recv()
            back_twin2(d, c).start()
        for d in range(2):
            back_twin2(d, c).wait_recv()
            V2[d * 256 : d * 256 + 256, cols(c)] = jnp.dot(
                C2[d * 256 : d * 256 + 256, :], RB[S2 + d * 640 : S2 + d * 640 + 640, cols(c)],
                preferred_element_type=F32,
            ).astype(BF)
            mixed2(d, c).start()

    @pl.loop(0, NC)
    def _(c):
        for n in (1, 2):
            tiles_back(n, c).wait_recv()
            back_twin1(n, c).start()

    @pl.loop(0, NC)
    def _(c):
        for n in range(3):
            back_twin1(n, c).wait_recv()

    @pl.loop(0, NC)
    def _(c):
        for d in range(2):
            mixed2(d, c).wait_recv()
            V1[d * 256 : d * 256 + 256, cols(c)] = jnp.dot(
                C1[d * 256 : d * 256 + 256, :], RB[S1 + d * 512 : S1 + d * 512 + 512, cols(c)],
                preferred_element_type=F32,
            ).astype(BF)
            mixed1(d, c).start()

    stat_twin().wait_recv()
    total = STC[0:8, :] + STC[8:16, :]
    count = 65536.0
    share = (total[0:1, :] / count) * (total[1:2, :] / count)
    aux[0, 0] = 256.0 * jnp.sum(share)

    @pl.loop(0, NC)
    def _(c):
        for d in range(2):
            mixed1(d, c).wait_recv()
        out[:, cols(c)] = jnp.dot(
            C0[...], RB[S0 : S0 + 768, cols(c)], preferred_element_type=F32
        ).astype(BF)

    @pl.loop(0, NC)
    def _(c):
        for u in range(2):
            tok_z(u, 0, c).wait_send()
            tok_z(u, 1, c).wait_send()
            slots_z(u, False, c).wait_send()
            slots_z(u, True, c).wait_send()
            back_z(u, False, c).wait_send()
            back_z(u, True, c).wait_send()
            back_twin2(u, c).wait_send()
            mixed2(u, c).wait_send()
            mixed1(u, c).wait_send()
        for idx in range(5):
            tok_twin(idx, c).wait_send()
        for n in range(3):
            back_twin1(n, c).wait_send()
        for idx in range(8):
            tiles_back(idx, c).wait_send()

    for n in range(9):
        meta_to(n).wait_send()
    for idx in range(8):
        tiles(idx).wait_send()
    remote(STA.at[0:120], STA.at[0:120], sts.at[0], str_.at[0], expert_2=kt).wait_send()
    remote(STB.at[0:56], STB.at[0:56], sts.at[1], str_.at[1], expert_2=kt).wait_send()
    stat_twin().wait_send()


def shards(tokens, routes, priority, router, w_in, w_out):
    anywhere = pl.BlockSpec(memory_space=pl.ANY)
    vmem = pl.BlockSpec(memory_space=pltpu.VMEM)
    dma = pltpu.SemaphoreType.DMA
    mixed, aux = pl.pallas_call(
        kernel,
        out_shape=(
            pltpu.VMEM((256, D), BF),
            jax.ShapeDtypeStruct((1, 1), F32),
        ),
        in_specs=[anywhere, vmem, vmem, anywhere, anywhere, anywhere],
        out_specs=(vmem, pl.BlockSpec(memory_space=pltpu.SMEM)),
        scratch_shapes=[
            pltpu.VMEM((10 * 256, D), BF),
            pltpu.VMEM((8 * 128, D), BF),
            pltpu.VMEM((2 * 192, D), BF),
            pltpu.VMEM((8 * 128, D), BF),
            pltpu.VMEM((8 * 128, D), BF),
            pltpu.VMEM((RB_ROWS, D), BF),
            pltpu.VMEM((2 * 256, D), BF),
            pltpu.VMEM((2 * 256, D), BF),
            pltpu.VMEM((D, FF), BF),
            pltpu.VMEM((D, FF), BF),
            pltpu.VMEM((D, 256), BF),
            pltpu.VMEM((3 * 128, FF), BF),
            pltpu.VMEM((2 * 128, 512), BF),
            pltpu.VMEM((2 * 192, 512), BF),
            pltpu.VMEM((2 * 256, 640), BF),
            pltpu.VMEM((2 * 256, 512), BF),
            pltpu.VMEM((256, 768), BF),
            pltpu.VMEM((10 * 8, 256), F32),
            pltpu.VMEM((16 * 8, 256), F32),
            pltpu.VMEM((8 * 8, 256), F32),
            pltpu.VMEM((2 * 8, 256), F32),
            dma((4,)),
            dma((2, 2, NC)), dma((2, 2, NC)),
            dma((5, NC)), dma((5, NC)),
            dma((2, 2, NC)), dma((2, 2, NC)),
            dma((9,)), dma((10,)),
            dma((8,)), dma((8,)),
            dma((8, NC)), dma((8, NC)),
            dma((3,)), dma((3,)),
            dma((2, 2, NC)), dma((2, 2, NC)),
            dma((2, NC)), dma((2, NC)),
            dma((3, NC)), dma((3, NC)),
            dma((2, NC)), dma((2, NC)),
            dma((2, NC)), dma((2, NC)),
        ],
        compiler_params=pltpu.CompilerParams(
            collective_id=0, has_side_effects=True, vmem_limit_bytes=64_000_000
        ),
    )(tokens, routes.T, priority, router, w_in[0], w_out[0])
    return mixed, aux[0, 0]


def solution(mesh):
    torus = Mesh(mesh.devices.reshape(4, 8, 2, mesh.shape["dp"]), EXPERT_DP)
    in_specs = (
        P(EXPERT_DP, None),
        P(EXPERT_DP, None),
        P(EXPERT_DP, None),
        P(),
        P(EXPERT_DP, None, None),
        P(EXPERT_DP, None, None),
    )
    return jax.shard_map(
        shards, mesh=torus, in_specs=in_specs, out_specs=(P(EXPERT_DP, None), P()), check_vma=False
    )
```
